32 devices in a mesh: row: 4 (over y, core), col: 8 (over z, x).
Axes of the slice: x: 2, y: 2, z: 4, core: 2. Of those that a mesh axis runs over, the one named last changes fastest.
Arguments:
- parent_front: float32 [8, 1024, 4, 2048], P(None, 'row', None, 'col'), may hold values from -6 to 6
- generators: bfloat16 [48, 256, 256], P('row'), may hold values from -1.5 to 1.5
- diagonal_blocks: bfloat16 [48, 256, 256], P('row'), may hold values from -6 to 6
- coupling: bfloat16 [2, 256, 256], replicated, may hold values from -0.375 to 0.375
- block_map: int32 [2, 24], replicated, may hold values from 0 to 31, as said below
- valid_rows: int32 [2, 24], replicated, may hold values from 128 to 256
Outputs:
- assembled: float32 [8, 1024, 4, 2048], P(None, 'row', None, 'col')
The draws below stay inside these ranges and needn't reach their ends.
Inputs may be any that keep to these rules, and one draw needn't show every extreme that they name: `block_map`: for each child c and each s < 2, the child blocks s * 12 to (s + 1) * 12 - 1 map in increasing order to distinct parent blocks of the range s * 16 to (s + 1) * 16 - 1, and the parent blocks s * 16 + m * 4 of that range always receive one.
All inputs are finite; a program needn't handle non-finite values.
Results may differ from the reference program's by a relative error of at most 0.0028.
Values may be sent and summed in bfloat16 or wider, within the bound.
A program may use at most 128 MiB of HBM per device.

```python
import jax
import jax.numpy as jnp
from jax import lax

BLK = 256
RANK = 256
BR_DEV = 8
PB = 32
BC_DEV = 4
WIN = 16
CG = 12
HALF = 2
CB = 24
N_ROW = 4
N_COL = 8


def draw_block_map(key, part):
    child_rows = []
    for child_index in range(2):
        pieces = []
        for group_index in range(HALF):
            window_key = jax.random.fold_in(key, 1000 * child_index + group_index + 17)
            offsets = jnp.arange(WIN, dtype=jnp.int32)
            scores = jax.random.randint(window_key, (WIN,), 0, 1 << 20, dtype=jnp.int32) * WIN + offsets
            scores = jnp.where(offsets % N_ROW == 0, jnp.int32(1 << 30), scores)
            gap_order = jnp.argsort(scores, stable=True)
            gap_slots = gap_order[:WIN - CG]
            gap_flags = jnp.zeros((WIN,), jnp.int32).at[gap_slots].set(1)
            sorted_slots = jnp.argsort(gap_flags * WIN + offsets, stable=True).astype(jnp.int32)
            chosen = sorted_slots[:CG] + WIN * group_index
            pieces.append(chosen)
        child_rows.append(jnp.concatenate(pieces))
    return jnp.stack(child_rows).astype(jnp.int32)


def place_ends(entries, own_key, low, high):
    longest = entries.shape.index(max(entries.shape))
    spots = []
    for shift in (0, 1):
        where = [jax.random.randint(jax.random.fold_in(own_key, axis), (), 0, length) for axis, length in enumerate(entries.shape)]
        where[longest] = (where[longest] + shift) % entries.shape[longest]
        spots.append(tuple(where))
    return entries.at[spots[0]].set(low).at[spots[1]].set(high)


def shard_levels(own_key, extent, cuts, smallest, largest):
    def one(dim, blocks):
        heights = jax.random.uniform(jax.random.fold_in(jax.random.fold_in(own_key, 6), dim), (blocks,), jnp.float32, smallest / len(cuts), largest / len(cuts))
        return jnp.repeat(jnp.exp(heights), extent[dim] // blocks).reshape((-1,) + (1,) * (len(extent) - dim - 1))

    loudness = one(*cuts[0])
    for cut in cuts[1:]:
        loudness = loudness * one(*cut)
    return loudness


def bell_draw(stream_key, dims, scale, reach, cuts=(), held_as=jnp.bfloat16):
    entries = jax.random.normal(stream_key, dims, jnp.float32) * scale
    if len(cuts) > 0:
        entries = shard_levels(stream_key, dims, cuts, -0.22, 0.18) * entries
    return jnp.clip(entries, min=-reach, max=reach).astype(held_as)


def setup_inputs(seed: int = 0) -> dict:
    arg_keys = jax.random.split(jax.random.key(seed), 7)
    parent_front = bell_draw(arg_keys[0], (BR_DEV, N_ROW * BLK, BC_DEV, N_COL * BLK), 1.0, 6.0, ((1, 4), (3, 8)), jnp.float32)
    generators = bell_draw(arg_keys[1], (2 * CB, BLK, RANK), 0.25, 1.5, ((0, 4),))
    diagonal_blocks = bell_draw(arg_keys[2], (2 * CB, BLK, BLK), 1.0, 6.0, ((0, 4),))
    coupling = bell_draw(arg_keys[3], (2, RANK, RANK), RANK ** -0.5, 0.375)
    block_map = draw_block_map(jax.random.fold_in(arg_keys[6], 71), 0)
    valid_rows = place_ends(jax.random.randint(arg_keys[5], (2, CB), BLK // 2, BLK + 1), jax.random.fold_in(arg_keys[5], 1), BLK // 2, BLK).astype(jnp.int32)
    return dict(parent_front=parent_front, generators=generators, diagonal_blocks=diagonal_blocks, coupling=coupling, block_map=block_map, valid_rows=valid_rows)


def child_select(stacked, child_index):
    grouped = stacked.reshape((HALF, 2, CG) + stacked.shape[1:])
    return grouped[:, child_index].reshape((CB,) + stacked.shape[1:])


def child_parts(gen_blocks, diag_rows, coupling_one, map_row, count_row):
    row_offsets = jnp.arange(BLK, dtype=jnp.int32)
    kept_mask = (row_offsets[None, :] < count_row[:, None]).astype(jnp.float32)
    masked = gen_blocks.astype(jnp.float32) * kept_mask[:, :, None]
    projected = jnp.einsum("ixq,qr->ixr", masked, coupling_one.astype(jnp.float32)).astype(jnp.bfloat16)
    diag_kept = diag_rows.astype(jnp.float32) * kept_mask[:, :, None] * kept_mask[:, None, :]
    placing = (map_row[None, :] == jnp.arange(PB, dtype=jnp.int32)[:, None]).astype(jnp.float32)
    placed_gen = jnp.einsum("pi,ixq->pxq", placing, masked)
    placed_proj = jnp.einsum("pi,ixq->pxq", placing, projected.astype(jnp.float32))
    placed_diag = jnp.einsum("pi,ixz->pxz", placing, diag_kept)
    return placed_gen, placed_proj, placed_diag


def reference(parent_front, generators, diagonal_blocks, coupling, block_map, valid_rows):
    front_blocks = parent_front.reshape(PB, BLK, PB, BLK)
    child_data = [child_parts(child_select(generators, child_index),
                              child_select(diagonal_blocks, child_index),
                              coupling[child_index], block_map[child_index], valid_rows[child_index])
                  for child_index in range(2)]
    placed_gen = jnp.stack([child_data[0][0], child_data[1][0]], axis=1)
    placed_proj = jnp.stack([child_data[0][1], child_data[1][1]])
    placed_diag = jnp.stack([child_data[0][2], child_data[1][2]], axis=1)
    block_ids = jnp.arange(PB, dtype=jnp.int32)

    def one_row(row_items):
        front_row, gen_row, diag_row, row_id = row_items
        on_diag = (block_ids == row_id).astype(jnp.float32)
        running = front_row
        for child_index in range(2):
            child_tile = jnp.einsum("xq,jzq->xjz", gen_row[child_index], placed_proj[child_index])
            child_tile = child_tile + diag_row[child_index][:, None, :] * on_diag[None, :, None]
            rounded = lax.optimization_barrier(child_tile.astype(jnp.bfloat16))
            running = running + rounded.astype(jnp.float32)
        return running

    rows_out = lax.map(one_row, (front_blocks, placed_gen, placed_diag, block_ids))
    return rows_out.reshape(BR_DEV, N_ROW * BLK, BC_DEV, N_COL * BLK)
```

```python
import functools

import jax
import jax.numpy as jnp
from jax import lax
from jax.experimental import pallas as pl
from jax.experimental.pallas import tpu as pltpu
from jax.sharding import PartitionSpec as P

MESH = pl.DeviceIdType.MESH
QUAD = 4


def exchange_kernel(
    row_count, col_count, row_cap, col_cap,
    gen_ref, diag_ref, coupling_ref, map_ref, count_ref,
    rows_out, cols_out, diag_out,
    send_rows, send_pair, rows_raw, cols_raw, diag_raw,
    far_send, far_recv, quad_send, quad_recv, pair_send, pair_recv,
    col_send, col_recv, fwd_send, fwd_recv, diag_send, diag_recv,
):
    groups = row_count // 2
    group_blocks, block, rank = gen_ref.shape
    window = row_cap * row_count
    chunk = row_cap * block // QUAD
    row = lax.axis_index("row")
    col = lax.axis_index("col")
    group = row // 2
    core = row % 2
    quarter = col % QUAD
    pair_row = group * 2 + 1 - core
    diag_row = col % row_count
    quad_cols = (
        col + 1 - 2 * (quarter % 2),
        col + 2 - 4 * (quarter // 2),
        col + 3 - 2 * quarter,
    )

    def lookup(child, source, slot):
        found = jnp.int32(0)
        count = jnp.int32(0)
        target = source * window + slot
        for k in range(group_blocks):
            hit = map_ref[child, source * group_blocks + k] == target
            found = jnp.where(hit, k, found)
            count = jnp.where(hit, count_ref[child, source * group_blocks + k], count)
        return found, count

    def remote(src, dst, send, recv, to_row, to_col):
        return pltpu.make_async_remote_copy(
            src_ref=src, dst_ref=dst, send_sem=send, recv_sem=recv,
            device_id=(to_row, to_col), device_id_type=MESH,
        )

    barrier = pltpu.get_barrier_semaphore()
    for k in range(1, row_count):
        pl.semaphore_signal(
            barrier, inc=1, device_id=((row + k) % row_count, col), device_id_type=MESH
        )
    for other in quad_cols:
        pl.semaphore_signal(barrier, inc=1, device_id=(row, other), device_id_type=MESH)

    start_row = quarter * chunk
    quarter_slot = start_row // block
    quarter_off = pl.multiple_of(start_row % block, chunk)
    for k in range(1, groups):
        dest = (group + k) % groups
        for r in range(2):
            found, _ = lookup(core, group, quarter_slot * row_count + 2 * dest + r)
            send_rows[k - 1, r] = gen_ref[found, pl.ds(quarter_off, chunk), :]
    for t in range(col_cap):
        found, _ = lookup(core, group, t * col_count + col)
        cols_raw[core, group, pl.ds(t * block, block), :] = gen_ref[found]
        diag_raw[core, group, pl.ds(t * block, block), :] = diag_ref[found]

    pl.semaphore_wait(barrier, row_count - 1 + QUAD - 1)

    sends = []

    def far_copy(k, r, child, source, dest_row):
        return remote(
            send_rows.at[k - 1, r], rows_raw.at[child, source, quarter],
            far_send.at[k - 1, r], far_recv.at[k - 1, child], dest_row, col,
        )

    for k in range(1, groups):
        dest = (group + k) % groups
        for r in range(2):
            copy = far_copy(k, r, core, group, 2 * dest + r)
            copy.start()
            sends.append(copy)

    own_cols = cols_raw.at[core, group]
    for k in range(1, groups):
        dest = (group + k) % groups
        copy = remote(own_cols, own_cols, col_send.at[k], col_recv.at[k], 2 * dest + core, col)
        copy.start()
        sends.append(copy)
    copy = remote(own_cols, own_cols, col_send.at[0], col_recv.at[0], pair_row, col)
    copy.start()
    sends.append(copy)

    own_diag = diag_raw.at[core, group]
    diag_away = remote(
        own_diag, own_diag, diag_send, diag_recv.at[core, group], diag_row, col
    )

    @pl.when(row != diag_row)
    def _():
        diag_away.start()

    for m in range(row_cap):
        found, _ = lookup(core, group, m * row_count + pair_row)
        send_pair[pl.ds(m * block, block), :] = gen_ref[found]
    for j in range(QUAD):
        slot, off = j * chunk // block, j * chunk % block
        found, _ = lookup(core, group, slot * row_count + row)
        rows_raw[core, group, j] = gen_ref[found, off:off + chunk, :]
    for j in range(QUAD):
        copy = remote(
            send_pair.at[pl.ds(j * chunk, chunk)], rows_raw.at[core, group, j],
            pair_send.at[j], pair_recv.at[j], pair_row, col,
        )
        copy.start()
        sends.append(copy)

    row_iota = lax.broadcasted_iota(jnp.int32, (block, rank), 0)
    col_iota = lax.broadcasted_iota(jnp.int32, (block, block), 1)

    def finish_rows(child, source, j):
        slot, off = j * chunk // block, j * chunk % block
        _, count = lookup(child, source, slot * row_count + row)
        kept = (row_iota[off:off + chunk] < count).astype(jnp.float32).astype(jnp.bfloat16)
        rows_out[source, j, :, child * rank:(child + 1) * rank] = rows_raw[child, source, j] * kept

    def finish_cols(child, source):
        for t in range(col_cap):
            _, count = lookup(child, source, t * col_count + col)
            kept = (row_iota < count).astype(jnp.float32).astype(jnp.bfloat16)
            masked = cols_raw[child, source, t * block:(t + 1) * block, :] * kept
            cols_out[source, t, :, child * rank:(child + 1) * rank] = jnp.dot(
                masked, coupling_ref[child], preferred_element_type=jnp.float32
            ).astype(jnp.bfloat16)

    for k in range(1, groups):
        source = (group + groups - k) % groups
        for child in range(2):
            far_copy(k, 0, child, source, row).wait_recv()
            landed = rows_raw.at[child, source, quarter]
            for j, other in enumerate(quad_cols):
                copy = remote(
                    landed, landed, quad_send.at[k - 1, child, j], quad_recv.at[k - 1, child, j],
                    row, other,
                )
                copy.start()
                sends.append(copy)

    for j in range(QUAD):
        remote(
            send_pair.at[pl.ds(j * chunk, chunk)], rows_raw.at[1 - core, group, j],
            pair_send.at[j], pair_recv.at[j], pair_row, col,
        ).wait_recv()
    for child in range(2):
        for j in range(QUAD):
            finish_rows(child, group, j)
    remote(own_cols, cols_raw.at[1 - core, group], col_send.at[0], col_recv.at[0], pair_row, col).wait_recv()
    for child in range(2):
        finish_cols(child, group)

    for k in range(1, groups):
        source = (group + groups - k) % groups
        landed = cols_raw.at[core, source]
        remote(own_cols, landed, col_send.at[k], col_recv.at[k], pair_row, col).wait_recv()
        copy = remote(landed, landed, fwd_send.at[k - 1], fwd_recv.at[k - 1], pair_row, col)
        copy.start()
        sends.append(copy)
    for k in range(1, groups):
        source = (group + groups - k) % groups
        remote(
            own_cols, cols_raw.at[1 - core, source], fwd_send.at[k - 1], fwd_recv.at[k - 1], pair_row, col
        ).wait_recv()
        for child in range(2):
            finish_cols(child, source)

    @pl.when(row == diag_row)
    def _():
        for source in range(groups):
            for child in range(2):
                @pl.when(2 * source + child != row)
                def _():
                    remote(
                        own_diag, diag_raw.at[child, source], diag_send, diag_recv.at[child, source],
                        pair_row, col,
                    ).wait_recv()
        for source in range(groups):
            for t in range(col_cap):
                total = jnp.zeros((block, block), jnp.float32)
                for child in range(2):
                    _, count = lookup(child, source, t * col_count + col)
                    inside = jnp.maximum(row_iota, col_iota) < count
                    piece = diag_raw[child, source, t * block:(t + 1) * block, :].astype(jnp.float32)
                    total = total + jnp.where(inside, piece, 0.0)
                diag_out[source, t] = total

    @pl.when(row != diag_row)
    def _():
        diag_out[...] = jnp.zeros_like(diag_out)

    for k in range(1, groups):
        source = (group + groups - k) % groups
        for child in range(2):
            for j, other in enumerate(quad_cols):
                landed = rows_raw.at[child, source, other % QUAD]
                remote(
                    landed, landed, quad_send.at[k - 1, child, j], quad_recv.at[k - 1, child, j],
                    row, other,
                ).wait_recv()
        for child in range(2):
            for j in range(QUAD):
                finish_rows(child, source, j)

    for copy in sends:
        copy.wait_send()

    @pl.when(row != diag_row)
    def _():
        diag_away.wait_send()


def shards(parent_front, generators, diagonal_blocks, coupling, block_map, valid_rows):
    row_count = lax.axis_size("row")
    col_count = lax.axis_size("col")
    groups = row_count // 2
    block, rank = generators.shape[1:]
    rows_local = parent_front.shape[0]
    cols_local = parent_front.shape[2]
    row_cap = rows_local // groups
    col_cap = cols_local // groups
    chunk = row_cap * block // QUAD
    vmem = pl.BlockSpec(memory_space=pltpu.VMEM)
    smem = pl.BlockSpec(memory_space=pltpu.SMEM)
    dma = pltpu.SemaphoreType.DMA
    rows, cols, diag = pl.pallas_call(
        functools.partial(exchange_kernel, row_count, col_count, row_cap, col_cap),
        out_shape=(
            jax.ShapeDtypeStruct((groups, QUAD, chunk, 2 * rank), jnp.bfloat16),
            jax.ShapeDtypeStruct((groups, col_cap, block, 2 * rank), jnp.bfloat16),
            jax.ShapeDtypeStruct((groups, col_cap, block, block), jnp.float32),
        ),
        in_specs=[vmem, vmem, vmem, smem, smem],
        out_specs=(vmem, vmem, vmem),
        scratch_shapes=[
            pltpu.VMEM((groups - 1, 2, chunk, rank), jnp.bfloat16),
            pltpu.VMEM((row_cap * block, rank), jnp.bfloat16),
            pltpu.VMEM((2, groups, QUAD, chunk, rank), jnp.bfloat16),
            pltpu.VMEM((2, groups, col_cap * block, rank), jnp.bfloat16),
            pltpu.VMEM((2, groups, col_cap * block, block), jnp.bfloat16),
            dma((groups - 1, 2)),
            dma((groups - 1, 2)),
            dma((groups - 1, 2, QUAD - 1)),
            dma((groups - 1, 2, QUAD - 1)),
            dma((QUAD,)),
            dma((QUAD,)),
            dma((groups,)),
            dma((groups,)),
            dma((groups - 1,)),
            dma((groups - 1,)),
            dma,
            dma((2, groups)),
        ],
        compiler_params=pltpu.CompilerParams(
            collective_id=0, has_side_effects=True, vmem_limit_bytes=48 * 1024 * 1024
        ),
    )(generators, diagonal_blocks, coupling, block_map, valid_rows)
    rows = rows.reshape(rows_local, block, 2 * rank)
    cols = cols.reshape(cols_local, block, 2 * rank)
    diag = diag.reshape(cols_local, block, block)
    row_parents = jnp.arange(rows_local, dtype=jnp.int32) * row_count + lax.axis_index("row")
    col_parents = jnp.arange(cols_local, dtype=jnp.int32) * col_count + lax.axis_index("col")
    on_diag = (row_parents[:, None] == col_parents[None, :]).astype(jnp.float32)
    tiles = jnp.einsum("axq,bzq->axbz", rows, cols, preferred_element_type=jnp.float32)
    placed = on_diag[:, None, :, None] * diag.transpose(1, 0, 2)[None]
    return parent_front + (tiles + placed)


def solution(mesh):
    in_specs = (
        P(None, "row", None, "col"),
        P("row", None, None),
        P("row", None, None),
        P(),
        P(),
        P(),
    )
    out_specs = P(None, "row", None, "col")
    return jax.shard_map(shards, mesh=mesh, in_specs=in_specs, out_specs=out_specs, check_vma=False)
```

```python
import functools

import jax
import jax.numpy as jnp
from jax import lax
from jax.experimental import pallas as pl
from jax.experimental.pallas import tpu as pltpu
from jax.sharding import PartitionSpec as P

MESH = pl.DeviceIdType.MESH
QUAD = 4
LANES = 128


def exchange_kernel(
    row_count, col_count, row_cap, col_cap,
    gen_hbm, diag_hbm, coupling_hbm, map_hbm, count_hbm,
    rows_out, cols_out, diag_out,
    gen_ref, diag_ref, coupling_ref, map_ref, count_ref, load_sem,
    send_rows, send_pair, rows_raw, cols_raw, diag_raw,
    far_send, far_recv, quad_send, quad_recv, pair_send, pair_recv,
    col_send, col_recv, fwd_send, fwd_recv, diag_send, diag_recv,
):
    groups = row_count // 2
    group_blocks, block, rank = gen_ref.shape
    window = row_cap * row_count
    chunk = row_cap * block // QUAD
    row = lax.axis_index("row")
    col = lax.axis_index("col")
    group = row // 2
    core = row % 2
    quarter = col % QUAD
    pair_row = group * 2 + 1 - core
    diag_row = col % row_count
    quad_cols = (
        col + 1 - 2 * (quarter % 2),
        col + 2 - 4 * (quarter // 2),
        col + 3 - 2 * quarter,
    )

    def lookup(child, source, slot):
        found = jnp.int32(0)
        count = jnp.int32(0)
        target = source * window + slot
        for k in range(group_blocks):
            hit = map_ref[child, source * group_blocks + k] == target
            found = jnp.where(hit, k, found)
            count = jnp.where(hit, count_ref[child, source * group_blocks + k], count)
        return found, count

    def remote(src, dst, send, recv, to_row, to_col):
        return pltpu.make_async_remote_copy(
            src_ref=src, dst_ref=dst, send_sem=send, recv_sem=recv,
            device_id=(to_row, to_col), device_id_type=MESH,
        )

    loads = [
        pltpu.make_async_copy(src, dst, load_sem.at[n])
        for n, (src, dst) in enumerate((
            (map_hbm, map_ref), (count_hbm, count_ref), (gen_hbm, gen_ref),
            (diag_hbm, diag_ref), (coupling_hbm, coupling_ref),
        ))
    ]
    for load in loads:
        load.start()

    barrier = pltpu.get_barrier_semaphore()
    for k in range(1, row_count):
        pl.semaphore_signal(
            barrier, inc=1, device_id=((row + k) % row_count, col), device_id_type=MESH
        )
    for other in quad_cols:
        pl.semaphore_signal(barrier, inc=1, device_id=(row, other), device_id_type=MESH)

    for load in loads:
        load.wait()
    start_row = quarter * chunk
    quarter_slot = start_row // block
    quarter_off = pl.multiple_of(start_row % block, chunk)
    for k in range(1, groups):
        dest = (group + k) % groups
        for r in range(2):
            found, _ = lookup(core, group, quarter_slot * row_count + 2 * dest + r)
            send_rows[k - 1, r] = gen_ref[found, pl.ds(quarter_off, chunk), :]
    for t in range(col_cap):
        found, _ = lookup(core, group, t * col_count + col)
        cols_raw[core, group, pl.ds(t * block, block), :] = gen_ref[found]
        diag_raw[core, group, pl.ds(t * block, block), :] = diag_ref[found]

    pl.semaphore_wait(barrier, row_count - 1 + QUAD - 1)

    sends = []

    def far_copy(k, r, child, source, dest_row):
        return remote(
            send_rows.at[k - 1, r], rows_raw.at[child, source, quarter],
            far_send.at[k - 1, r], far_recv.at[k - 1, child], dest_row, col,
        )

    for k in range(1, groups):
        dest = (group + k) % groups
        for r in range(2):
            copy = far_copy(k, r, core, group, 2 * dest + r)
            copy.start()
            sends.append(copy)

    own_cols = cols_raw.at[core, group]
    for k in range(1, groups):
        dest = (group + k) % groups
        copy = remote(own_cols, own_cols, col_send.at[k], col_recv.at[k], 2 * dest + core, col)
        copy.start()
        sends.append(copy)
    copy = remote(own_cols, own_cols, col_send.at[0], col_recv.at[0], pair_row, col)
    copy.start()
    sends.append(copy)

    own_diag = diag_raw.at[core, group]
    diag_away = remote(
        own_diag, own_diag, diag_send, diag_recv.at[core, group], diag_row, col
    )

    @pl.when(row != diag_row)
    def _():
        diag_away.start()

    for m in range(row_cap):
        found, _ = lookup(core, group, m * row_count + pair_row)
        send_pair[pl.ds(m * block, block), :] = gen_ref[found]
    for j in range(QUAD):
        slot, off = j * chunk // block, j * chunk % block
        found, _ = lookup(core, group, slot * row_count + row)
        rows_raw[core, group, j] = gen_ref[found, off:off + chunk, :]
    for j in range(QUAD):
        copy = remote(
            send_pair.at[pl.ds(j * chunk, chunk)], rows_raw.at[core, group, j],
            pair_send.at[j], pair_recv.at[j], pair_row, col,
        )
        copy.start()
        sends.append(copy)

    row_iota = lax.broadcasted_iota(jnp.int32, (block, rank), 0)
    col_iota = lax.broadcasted_iota(jnp.int32, (block, block), 1)

    def finish_rows(child, source, j):
        slot, off = j * chunk // block, j * chunk % block
        _, count = lookup(child, source, slot * row_count + row)
        kept = (row_iota[off:off + chunk] < count).astype(jnp.float32).astype(jnp.bfloat16)
        rows_out[source, j, :, child * rank:(child + 1) * rank] = rows_raw[child, source, j] * kept

    def finish_cols(child, source):
        for t in range(col_cap):
            _, count = lookup(child, source, t * col_count + col)
            kept = (row_iota < count).astype(jnp.float32).astype(jnp.bfloat16)
            masked = cols_raw[child, source, t * block:(t + 1) * block, :] * kept
            cols_out[source, t, child * rank:(child + 1) * rank, :] = lax.dot_general(
                coupling_ref[child], masked, (((0,), (1,)), ((), ())),
                preferred_element_type=jnp.float32,
            ).astype(jnp.bfloat16)

    for k in range(1, groups):
        source = (group + groups - k) % groups
        for child in range(2):
            far_copy(k, 0, child, source, row).wait_recv()
            landed = rows_raw.at[child, source, quarter]
            for j, other in enumerate(quad_cols):
                copy = remote(
                    landed, landed, quad_send.at[k - 1, child, j], quad_recv.at[k - 1, child, j],
                    row, other,
                )
                copy.start()
                sends.append(copy)

    for j in range(QUAD):
        remote(
            send_pair.at[pl.ds(j * chunk, chunk)], rows_raw.at[1 - core, group, j],
            pair_send.at[j], pair_recv.at[j], pair_row, col,
        ).wait_recv()
    for child in range(2):
        for j in range(QUAD):
            finish_rows(child, group, j)
    remote(own_cols, cols_raw.at[1 - core, group], col_send.at[0], col_recv.at[0], pair_row, col).wait_recv()
    for child in range(2):
        finish_cols(child, group)

    for k in range(1, groups):
        source = (group + groups - k) % groups
        landed = cols_raw.at[core, source]
        remote(own_cols, landed, col_send.at[k], col_recv.at[k], pair_row, col).wait_recv()
        copy = remote(landed, landed, fwd_send.at[k - 1], fwd_recv.at[k - 1], pair_row, col)
        copy.start()
        sends.append(copy)
    for k in range(1, groups):
        source = (group + groups - k) % groups
        remote(
            own_cols, cols_raw.at[1 - core, source], fwd_send.at[k - 1], fwd_recv.at[k - 1], pair_row, col
        ).wait_recv()
        for child in range(2):
            finish_cols(child, source)

    @pl.when(row == diag_row)
    def _():
        for source in range(groups):
            for child in range(2):
                @pl.when(2 * source + child != row)
                def _():
                    remote(
                        own_diag, diag_raw.at[child, source], diag_send, diag_recv.at[child, source],
                        pair_row, col,
                    ).wait_recv()
        for source in range(groups):
            for t in range(col_cap):
                total = jnp.zeros((block, block), jnp.float32)
                for child in range(2):
                    _, count = lookup(child, source, t * col_count + col)
                    inside = jnp.maximum(row_iota, col_iota) < count
                    piece = diag_raw[child, source, t * block:(t + 1) * block, :].astype(jnp.float32)
                    total = total + jnp.where(inside, piece, 0.0)
                diag_out[source, t] = total

    @pl.when(row != diag_row)
    def _():
        diag_out[...] = jnp.zeros_like(diag_out)

    for k in range(1, groups):
        source = (group + groups - k) % groups
        for child in range(2):
            for j, other in enumerate(quad_cols):
                landed = rows_raw.at[child, source, other % QUAD]
                remote(
                    landed, landed, quad_send.at[k - 1, child, j], quad_recv.at[k - 1, child, j],
                    row, other,
                ).wait_recv()
        for child in range(2):
            for j in range(QUAD):
                finish_rows(child, source, j)

    for copy in sends:
        copy.wait_send()

    @pl.when(row != diag_row)
    def _():
        diag_away.wait_send()


def add_kernel(row_count, col_count, front_ref, rows_ref, cols_ref, diag_ref, out_ref):
    cols_local, _, block = cols_ref.shape
    halves = block // LANES
    per_row = halves * cols_local
    row_parent = pl.program_id(0) * row_count + lax.axis_index("row")
    for b in range(cols_local):
        tile = jnp.dot(rows_ref[...], cols_ref[b], preferred_element_type=jnp.float32)
        for h in range(halves):
            spot = pl.ds(h * cols_local + b, block, stride=per_row)
            lanes = slice(h * LANES, (h + 1) * LANES)
            out_ref[spot, :] = front_ref[spot, :] + tile[:, lanes]

        @pl.when(row_parent == b * col_count + lax.axis_index("col"))
        def _():
            for h in range(halves):
                spot = pl.ds(h * cols_local + b, block, stride=per_row)
                out_ref[spot, :] = out_ref[spot, :] + diag_ref[b, :, h * LANES:(h + 1) * LANES]


def shards(parent_front, generators, diagonal_blocks, coupling, block_map, valid_rows):
    row_count = lax.axis_size("row")
    col_count = lax.axis_size("col")
    groups = row_count // 2
    block, rank = generators.shape[1:]
    rows_local = parent_front.shape[0]
    cols_local = parent_front.shape[2]
    row_cap = rows_local // groups
    col_cap = cols_local // groups
    chunk = row_cap * block // QUAD
    vmem = pl.BlockSpec(memory_space=pltpu.VMEM)
    hbm = pl.BlockSpec(memory_space=pltpu.HBM)
    dma = pltpu.SemaphoreType.DMA
    rows, cols, diag = pl.pallas_call(
        functools.partial(exchange_kernel, row_count, col_count, row_cap, col_cap),
        out_shape=(
            jax.ShapeDtypeStruct((groups, QUAD, chunk, 2 * rank), jnp.bfloat16),
            jax.ShapeDtypeStruct((groups, col_cap, 2 * rank, block), jnp.bfloat16),
            jax.ShapeDtypeStruct((groups, col_cap, block, block), jnp.float32),
        ),
        in_specs=[hbm] * 5,
        out_specs=(vmem, vmem, vmem),
        scratch_shapes=[
            pltpu.VMEM(generators.shape, jnp.bfloat16),
            pltpu.VMEM(diagonal_blocks.shape, jnp.bfloat16),
            pltpu.VMEM(coupling.shape, jnp.bfloat16),
            pltpu.SMEM(block_map.shape, jnp.int32),
            pltpu.SMEM(valid_rows.shape, jnp.int32),
            dma((5,)),
            pltpu.VMEM((groups - 1, 2, chunk, rank), jnp.bfloat16),
            pltpu.VMEM((row_cap * block, rank), jnp.bfloat16),
            pltpu.VMEM((2, groups, QUAD, chunk, rank), jnp.bfloat16),
            pltpu.VMEM((2, groups, col_cap * block, rank), jnp.bfloat16),
            pltpu.VMEM((2, groups, col_cap * block, block), jnp.bfloat16),
            dma((groups - 1, 2)),
            dma((groups - 1, 2)),
            dma((groups - 1, 2, QUAD - 1)),
            dma((groups - 1, 2, QUAD - 1)),
            dma((QUAD,)),
            dma((QUAD,)),
            dma((groups,)),
            dma((groups,)),
            dma((groups - 1,)),
            dma((groups - 1,)),
            dma,
            dma((2, groups)),
        ],
        compiler_params=pltpu.CompilerParams(
            collective_id=0, has_side_effects=True, vmem_limit_bytes=67_043_328
        ),
    )(generators, diagonal_blocks, coupling, block_map, valid_rows)
    rows = rows.reshape(rows_local, block, 2 * rank)
    cols = cols.reshape(cols_local, 2 * rank, block)
    diag = diag.reshape(cols_local, block, block)
    halves = block // LANES
    per_row = halves * cols_local
    flat = parent_front.reshape(rows_local, block, cols_local, halves, LANES)
    flat = flat.transpose(0, 1, 3, 2, 4).reshape(rows_local, block * per_row, LANES)
    flat_spec = pl.BlockSpec((None, block * per_row, LANES), lambda a: (a, 0, 0))
    out = pl.pallas_call(
        functools.partial(add_kernel, row_count, col_count),
        grid=(rows_local,),
        out_shape=jax.ShapeDtypeStruct(flat.shape, jnp.float32),
        in_specs=[
            flat_spec,
            pl.BlockSpec((None, block, 2 * rank), lambda a: (a, 0, 0)),
            pl.BlockSpec(cols.shape, lambda a: (0, 0, 0)),
            pl.BlockSpec(diag.shape, lambda a: (0, 0, 0)),
        ],
        out_specs=flat_spec,
    )(flat, rows, cols, diag)
    out = out.reshape(rows_local, block, halves, cols_local, LANES)
    return out.transpose(0, 1, 3, 2, 4).reshape(parent_front.shape)


def solution(mesh):
    in_specs = (
        P(None, "row", None, "col"),
        P("row", None, None),
        P("row", None, None),
        P(),
        P(),
        P(),
    )
    out_specs = P(None, "row", None, "col")
    return jax.shard_map(shards, mesh=mesh, in_specs=in_specs, out_specs=out_specs, check_vma=False)
```

```python
import functools

import jax
import jax.numpy as jnp
from jax import lax
from jax.experimental import pallas as pl
from jax.experimental.pallas import tpu as pltpu
from jax.sharding import PartitionSpec as P

MESH = pl.DeviceIdType.MESH
QUAD = 4
LANES = 128


def exchange_kernel(
    row_count, col_count, row_cap, col_cap,
    gen_hbm, diag_hbm, coupling_hbm, map_hbm, count_hbm, front_hbm,
    rows_out, cols_out, diag_out, front_out,
    gen_ref, diag_ref, coupling_ref, map_ref, count_ref, load_sem, front_sem,
    send_rows, send_pair, rows_raw, cols_raw, diag_raw,
    far_send, far_recv, quad_send, quad_recv, pair_send, pair_recv,
    col_send, col_recv, fwd_send, fwd_recv, diag_send, diag_recv,
):
    groups = row_count // 2
    group_blocks, block, rank = gen_ref.shape
    window = row_cap * row_count
    chunk = row_cap * block // QUAD
    row = lax.axis_index("row")
    col = lax.axis_index("col")
    group = row // 2
    core = row % 2
    quarter = col % QUAD
    pair_row = group * 2 + 1 - core
    diag_row = col % row_count
    quad_cols = (
        col + 1 - 2 * (quarter % 2),
        col + 2 - 4 * (quarter // 2),
        col + 3 - 2 * quarter,
    )

    def lookup(child, source, slot):
        found = jnp.int32(0)
        count = jnp.int32(0)
        target = source * window + slot
        for k in range(group_blocks):
            hit = map_ref[child, source * group_blocks + k] == target
            found = jnp.where(hit, k, found)
            count = jnp.where(hit, count_ref[child, source * group_blocks + k], count)
        return found, count

    def remote(src, dst, send, recv, to_row, to_col):
        return pltpu.make_async_remote_copy(
            src_ref=src, dst_ref=dst, send_sem=send, recv_sem=recv,
            device_id=(to_row, to_col), device_id_type=MESH,
        )

    loads = [
        pltpu.make_async_copy(src, dst, load_sem.at[n])
        for n, (src, dst) in enumerate((
            (map_hbm, map_ref), (count_hbm, count_ref), (gen_hbm, gen_ref),
            (diag_hbm, diag_ref), (coupling_hbm, coupling_ref),
        ))
    ]
    for load in loads:
        load.start()

    barrier = pltpu.get_barrier_semaphore()
    for k in range(1, row_count):
        pl.semaphore_signal(
            barrier, inc=1, device_id=((row + k) % row_count, col), device_id_type=MESH
        )
    for other in quad_cols:
        pl.semaphore_signal(barrier, inc=1, device_id=(row, other), device_id_type=MESH)

    for load in loads:
        load.wait()
    front_load = pltpu.make_async_copy(front_hbm, front_out, front_sem)
    front_load.start()
    start_row = quarter * chunk
    quarter_slot = start_row // block
    quarter_off = pl.multiple_of(start_row % block, chunk)
    for k in range(1, groups):
        dest = (group + k) % groups
        for r in range(2):
            found, _ = lookup(core, group, quarter_slot * row_count + 2 * dest + r)
            send_rows[k - 1, r] = gen_ref[found, pl.ds(quarter_off, chunk), :]
    for t in range(col_cap):
        found, _ = lookup(core, group, t * col_count + col)
        cols_raw[core, group, pl.ds(t * block, block), :] = gen_ref[found]
        diag_raw[core, group, pl.ds(t * block, block), :] = diag_ref[found]

    pl.semaphore_wait(barrier, row_count - 1 + QUAD - 1)

    sends = []

    def far_copy(k, r, child, source, dest_row):
        return remote(
            send_rows.at[k - 1, r], rows_raw.at[child, source, quarter],
            far_send.at[k - 1, r], far_recv.at[k - 1, child], dest_row, col,
        )

    for k in range(1, groups):
        dest = (group + k) % groups
        for r in range(2):
            copy = far_copy(k, r, core, group, 2 * dest + r)
            copy.start()
            sends.append(copy)

    own_cols = cols_raw.at[core, group]
    for k in range(1, groups):
        dest = (group + k) % groups
        copy = remote(own_cols, own_cols, col_send.at[k], col_recv.at[k], 2 * dest + core, col)
        copy.start()
        sends.append(copy)
    copy = remote(own_cols, own_cols, col_send.at[0], col_recv.at[0], pair_row, col)
    copy.start()
    sends.append(copy)

    own_diag = diag_raw.at[core, group]
    diag_away = remote(
        own_diag, own_diag, diag_send, diag_recv.at[core, group], diag_row, col
    )

    @pl.when(row != diag_row)
    def _():
        diag_away.start()

    for m in range(row_cap):
        found, _ = lookup(core, group, m * row_count + pair_row)
        send_pair[pl.ds(m * block, block), :] = gen_ref[found]
    for j in range(QUAD):
        slot, off = j * chunk // block, j * chunk % block
        found, _ = lookup(core, group, slot * row_count + row)
        rows_raw[core, group, j] = gen_ref[found, off:off + chunk, :]
    for j in range(QUAD):
        copy = remote(
            send_pair.at[pl.ds(j * chunk, chunk)], rows_raw.at[core, group, j],
            pair_send.at[j], pair_recv.at[j], pair_row, col,
        )
        copy.start()
        sends.append(copy)

    row_iota = lax.broadcasted_iota(jnp.int32, (block, rank), 0)
    col_iota = lax.broadcasted_iota(jnp.int32, (block, block), 1)

    def finish_rows(child, source, j):
        slot, off = j * chunk // block, j * chunk % block
        _, count = lookup(child, source, slot * row_count + row)
        kept = (row_iota[off:off + chunk] < count).astype(jnp.float32).astype(jnp.bfloat16)
        rows_out[source, j, :, child * rank:(child + 1) * rank] = rows_raw[child, source, j] * kept

    def finish_cols(child, source):
        for t in range(col_cap):
            _, count = lookup(child, source, t * col_count + col)
            kept = (row_iota < count).astype(jnp.float32).astype(jnp.bfloat16)
            masked = cols_raw[child, source, t * block:(t + 1) * block, :] * kept
            cols_out[source, t, child * rank:(child + 1) * rank, :] = lax.dot_general(
                coupling_ref[child], masked, (((0,), (1,)), ((), ())),
                preferred_element_type=jnp.float32,
            ).astype(jnp.bfloat16)

    for k in range(1, groups):
        source = (group + groups - k) % groups
        for child in range(2):
            far_copy(k, 0, child, source, row).wait_recv()
            landed = rows_raw.at[child, source, quarter]
            for j, other in enumerate(quad_cols):
                copy = remote(
                    landed, landed, quad_send.at[k - 1, child, j], quad_recv.at[k - 1, child, j],
                    row, other,
                )
                copy.start()
                sends.append(copy)

    for j in range(QUAD):
        remote(
            send_pair.at[pl.ds(j * chunk, chunk)], rows_raw.at[1 - core, group, j],
            pair_send.at[j], pair_recv.at[j], pair_row, col,
        ).wait_recv()
    for child in range(2):
        for j in range(QUAD):
            finish_rows(child, group, j)
    remote(own_cols, cols_raw.at[1 - core, group], col_send.at[0], col_recv.at[0], pair_row, col).wait_recv()
    for child in range(2):
        finish_cols(child, group)

    for k in range(1, groups):
        source = (group + groups - k) % groups
        landed = cols_raw.at[core, source]
        remote(own_cols, landed, col_send.at[k], col_recv.at[k], pair_row, col).wait_recv()
        copy = remote(landed, landed, fwd_send.at[k - 1], fwd_recv.at[k - 1], pair_row, col)
        copy.start()
        sends.append(copy)
    for k in range(1, groups):
        source = (group + groups - k) % groups
        remote(
            own_cols, cols_raw.at[1 - core, source], fwd_send.at[k - 1], fwd_recv.at[k - 1], pair_row, col
        ).wait_recv()
        for child in range(2):
            finish_cols(child, source)

    @pl.when(row == diag_row)
    def _():
        for source in range(groups):
            for child in range(2):
                @pl.when(2 * source + child != row)
                def _():
                    remote(
                        own_diag, diag_raw.at[child, source], diag_send, diag_recv.at[child, source],
                        pair_row, col,
                    ).wait_recv()
        for source in range(groups):
            for t in range(col_cap):
                total = jnp.zeros((block, block), jnp.float32)
                for child in range(2):
                    _, count = lookup(child, source, t * col_count + col)
                    inside = jnp.maximum(row_iota, col_iota) < count
                    piece = diag_raw[child, source, t * block:(t + 1) * block, :].astype(jnp.float32)
                    total = total + jnp.where(inside, piece, 0.0)
                diag_out[source, t] = total

    @pl.when(row != diag_row)
    def _():
        diag_out[...] = jnp.zeros_like(diag_out)

    for k in range(1, groups):
        source = (group + groups - k) % groups
        for child in range(2):
            for j, other in enumerate(quad_cols):
                landed = rows_raw.at[child, source, other % QUAD]
                remote(
                    landed, landed, quad_send.at[k - 1, child, j], quad_recv.at[k - 1, child, j],
                    row, other,
                ).wait_recv()
        for child in range(2):
            for j in range(QUAD):
                finish_rows(child, source, j)

    front_load.wait()
    for copy in sends:
        copy.wait_send()

    @pl.when(row != diag_row)
    def _():
        diag_away.wait_send()


def add_kernel(
    row_count, col_count, front_ref, rows_ref, cols_ref, diag_ref, out_ref, staged, out_sem
):
    rows_local = rows_ref.shape[0]
    cols_local, _, block = cols_ref.shape
    halves = block // LANES
    per_row = halves * cols_local
    row = lax.axis_index("row")
    col = lax.axis_index("col")

    def write(a):
        return pltpu.make_async_copy(staged.at[a % 2], out_ref.at[a], out_sem.at[a % 2])

    for a in range(rows_local):
        if a >= 2:
            write(a - 2).wait()
        for b in range(cols_local):
            tile = jnp.dot(rows_ref[a], cols_ref[b], preferred_element_type=jnp.float32)
            for h in range(halves):
                spot = pl.ds(h * cols_local + b, block, stride=per_row)
                staged[a % 2, spot, :] = front_ref[a, spot, :] + tile[:, h * LANES:(h + 1) * LANES]
        row_parent = a * row_count + row

        @pl.when(row_parent % col_count == col)
        def _():
            b = row_parent // col_count
            for h in range(halves):
                spot = pl.ds(h * cols_local + b, block, stride=per_row)
                piece = diag_ref[b, :, h * LANES:(h + 1) * LANES]
                staged[a % 2, spot, :] = staged[a % 2, spot, :] + piece

        write(a).start()
    for a in range(rows_local - 2, rows_local):
        write(a).wait()


def shards(parent_front, generators, diagonal_blocks, coupling, block_map, valid_rows):
    row_count = lax.axis_size("row")
    col_count = lax.axis_size("col")
    groups = row_count // 2
    block, rank = generators.shape[1:]
    rows_local = parent_front.shape[0]
    cols_local = parent_front.shape[2]
    row_cap = rows_local // groups
    col_cap = cols_local // groups
    chunk = row_cap * block // QUAD
    vmem = pl.BlockSpec(memory_space=pltpu.VMEM)
    hbm = pl.BlockSpec(memory_space=pltpu.HBM)
    dma = pltpu.SemaphoreType.DMA
    halves = block // LANES
    per_row = halves * cols_local
    flat = parent_front.reshape(rows_local, block, cols_local, halves, LANES)
    flat = flat.transpose(0, 1, 3, 2, 4).reshape(rows_local, block * per_row, LANES)
    operands = [
        pltpu.with_memory_space_constraint(x, pltpu.HBM)
        for x in (generators, diagonal_blocks, coupling, block_map, valid_rows, flat)
    ]
    rows, cols, diag, front = pl.pallas_call(
        functools.partial(exchange_kernel, row_count, col_count, row_cap, col_cap),
        out_shape=(
            pltpu.VMEM((groups, QUAD, chunk, 2 * rank), jnp.bfloat16),
            pltpu.VMEM((groups, col_cap, 2 * rank, block), jnp.bfloat16),
            pltpu.VMEM((groups, col_cap, block, block), jnp.float32),
            pltpu.VMEM(flat.shape, jnp.float32),
        ),
        in_specs=[hbm] * 6,
        out_specs=(vmem,) * 4,
        scratch_shapes=[
            pltpu.VMEM(generators.shape, jnp.bfloat16),
            pltpu.VMEM(diagonal_blocks.shape, jnp.bfloat16),
            pltpu.VMEM(coupling.shape, jnp.bfloat16),
            pltpu.SMEM(block_map.shape, jnp.int32),
            pltpu.SMEM(valid_rows.shape, jnp.int32),
            dma((5,)),
            dma,
            pltpu.VMEM((groups - 1, 2, chunk, rank), jnp.bfloat16),
            pltpu.VMEM((row_cap * block, rank), jnp.bfloat16),
            pltpu.VMEM((2, groups, QUAD, chunk, rank), jnp.bfloat16),
            pltpu.VMEM((2, groups, col_cap * block, rank), jnp.bfloat16),
            pltpu.VMEM((2, groups, col_cap * block, block), jnp.bfloat16),
            dma((groups - 1, 2)),
            dma((groups - 1, 2)),
            dma((groups - 1, 2, QUAD - 1)),
            dma((groups - 1, 2, QUAD - 1)),
            dma((QUAD,)),
            dma((QUAD,)),
            dma((groups,)),
            dma((groups,)),
            dma((groups - 1,)),
            dma((groups - 1,)),
            dma,
            dma((2, groups)),
        ],
        compiler_params=pltpu.CompilerParams(
            collective_id=0, has_side_effects=True, vmem_limit_bytes=32 * 1024 * 1024
        ),
    )(*operands)
    rows = rows.reshape(rows_local, block, 2 * rank)
    cols = cols.reshape(cols_local, 2 * rank, block)
    diag = diag.reshape(cols_local, block, block)
    out = pl.pallas_call(
        functools.partial(add_kernel, row_count, col_count),
        out_shape=jax.ShapeDtypeStruct(flat.shape, jnp.float32),
        in_specs=[vmem] * 4,
        out_specs=hbm,
        scratch_shapes=[pltpu.VMEM((2,) + flat.shape[1:], jnp.float32), dma((2,))],
        compiler_params=pltpu.CompilerParams(vmem_limit_bytes=32 * 1024 * 1024),
    )(*(pltpu.with_memory_space_constraint(x, pltpu.VMEM) for x in (front, rows, cols, diag)))
    out = out.reshape(rows_local, block, halves, cols_local, LANES)
    return out.transpose(0, 1, 3, 2, 4).reshape(parent_front.shape)


def solution(mesh):
    in_specs = (
        P(None, "row", None, "col"),
        P("row", None, None),
        P("row", None, None),
        P(),
        P(),
        P(),
    )
    out_specs = P(None, "row", None, "col")
    return jax.shard_map(shards, mesh=mesh, in_specs=in_specs, out_specs=out_specs, check_vma=False)
```

```python
import functools

import jax
import jax.numpy as jnp
from jax import lax
from jax.experimental import pallas as pl
from jax.experimental.pallas import tpu as pltpu
from jax.sharding import PartitionSpec as P

MESH = pl.DeviceIdType.MESH
QUAD = 4
LANES = 128


def exchange_kernel(
    row_count, col_count, row_cap, col_cap,
    gen_hbm, diag_hbm, coupling_hbm, map_hbm, count_hbm, front_hbm,
    rows_out, cols_out, diag_out, front_out,
    gen_ref, diag_ref, coupling_ref, map_ref, count_ref, load_sem, front_sem,
    send_rows, send_pair, rows_raw, cols_raw, diag_raw,
    far_send, far_recv, quad_send, quad_recv, pair_send, pair_recv,
    col_send, col_recv, fwd_send, fwd_recv, diag_send, diag_recv, own_send, own_recv,
):
    groups = row_count // 2
    group_blocks, block, rank = gen_ref.shape
    window = row_cap * row_count
    chunk = row_cap * block // QUAD
    row = lax.axis_index("row")
    col = lax.axis_index("col")
    group = row // 2
    core = row % 2
    quarter = col % QUAD
    pair_row = group * 2 + 1 - core
    diag_row = col % row_count
    quad_cols = (
        col + 1 - 2 * (quarter % 2),
        col + 2 - 4 * (quarter // 2),
        col + 3 - 2 * quarter,
    )

    def lookup(child, source, slot):
        found = jnp.int32(0)
        count = jnp.int32(0)
        target = source * window + slot
        for k in range(group_blocks):
            hit = map_ref[child, source * group_blocks + k] == target
            found = jnp.where(hit, k, found)
            count = jnp.where(hit, count_ref[child, source * group_blocks + k], count)
        return found, count

    def remote(src, dst, send, recv, to_row, to_col):
        return pltpu.make_async_remote_copy(
            src_ref=src, dst_ref=dst, send_sem=send, recv_sem=recv,
            device_id=(to_row, to_col), device_id_type=MESH,
        )

    loads = [
        pltpu.make_async_copy(src, dst, load_sem.at[n])
        for n, (src, dst) in enumerate((
            (map_hbm, map_ref), (count_hbm, count_ref), (gen_hbm, gen_ref),
            (diag_hbm, diag_ref), (coupling_hbm, coupling_ref),
        ))
    ]
    for load in loads:
        load.start()

    barrier = pltpu.get_barrier_semaphore()
    for k in range(1, row_count):
        pl.semaphore_signal(
            barrier, inc=1, device_id=((row + k) % row_count, col), device_id_type=MESH
        )
    for other in quad_cols:
        pl.semaphore_signal(barrier, inc=1, device_id=(row, other), device_id_type=MESH)

    for load in loads:
        load.wait()
    front_load = pltpu.make_async_copy(front_hbm, front_out, front_sem)
    front_load.start()
    start_row = quarter * chunk
    quarter_slot = start_row // block
    quarter_off = pl.multiple_of(start_row % block, chunk)
    for k in range(1, groups):
        dest = (group + k) % groups
        for r in range(2):
            found, _ = lookup(core, group, quarter_slot * row_count + 2 * dest + r)
            send_rows[k - 1, r] = gen_ref[found, pl.ds(quarter_off, chunk), :]
    for t in range(col_cap):
        found, _ = lookup(core, group, t * col_count + col)
        cols_raw[core, group, pl.ds(t * block, block), :] = gen_ref[found]
        diag_raw[core, group, pl.ds(t * block, block), :] = diag_ref[found]

    pl.semaphore_wait(barrier, row_count - 1 + QUAD - 1)

    sends = []

    def far_copy(k, r, child, source, dest_row):
        return remote(
            send_rows.at[k - 1, r], rows_raw.at[child, source, quarter],
            far_send.at[k - 1, r], far_recv.at[k - 1, child], dest_row, col,
        )

    for k in range(1, groups):
        dest = (group + k) % groups
        for r in range(2):
            copy = far_copy(k, r, core, group, 2 * dest + r)
            copy.start()
            sends.append(copy)

    own_cols = cols_raw.at[core, group]
    col_away = []
    for k in range(1, groups):
        dest = (group + k) % groups
        copy = remote(own_cols, own_cols, col_send.at[k], col_recv.at[k], 2 * dest + core, col)
        pl.when(diag_row // 2 != dest)(copy.start)
        col_away.append((dest, copy))
    copy = remote(own_cols, own_cols, col_send.at[0], col_recv.at[0], pair_row, col)
    copy.start()
    sends.append(copy)

    own_diag = diag_raw.at[core, group]
    diag_away = remote(
        own_diag, own_diag, diag_send, diag_recv.at[core, group], diag_row, col
    )

    @pl.when(row != diag_row)
    def _():
        diag_away.start()

    for m in range(row_cap):
        found, _ = lookup(core, group, m * row_count + pair_row)
        send_pair[pl.ds(m * block, block), :] = gen_ref[found]
    for j in range(QUAD):
        slot, off = j * chunk // block, j * chunk % block
        found, _ = lookup(core, group, slot * row_count + row)
        rows_raw[core, group, j] = gen_ref[found, off:off + chunk, :]
    for j in range(QUAD):
        copy = remote(
            send_pair.at[pl.ds(j * chunk, chunk)], rows_raw.at[core, group, j],
            pair_send.at[j], pair_recv.at[j], pair_row, col,
        )
        copy.start()
        sends.append(copy)

    row_iota = lax.broadcasted_iota(jnp.int32, (block, rank), 0)
    col_iota = lax.broadcasted_iota(jnp.int32, (block, block), 1)

    def finish_rows(child, source, j):
        slot, off = j * chunk // block, j * chunk % block
        _, count = lookup(child, source, slot * row_count + row)
        kept = (row_iota[off:off + chunk] < count).astype(jnp.float32).astype(jnp.bfloat16)
        rows_out[source, j, :, child * rank:(child + 1) * rank] = rows_raw[child, source, j] * kept

    def finish_cols(child, source):
        for t in range(col_cap):
            _, count = lookup(child, source, t * col_count + col)
            kept = (row_iota < count).astype(jnp.float32).astype(jnp.bfloat16)
            masked = cols_raw[child, source, t * block:(t + 1) * block, :] * kept
            cols_out[source, t, child * rank:(child + 1) * rank, :] = lax.dot_general(
                coupling_ref[child], masked, (((0,), (1,)), ((), ())),
                preferred_element_type=jnp.float32,
            ).astype(jnp.bfloat16)

    for k in range(1, groups):
        source = (group + groups - k) % groups
        for child in range(2):
            far_copy(k, 0, child, source, row).wait_recv()
            landed = rows_raw.at[child, source, quarter]
            for j, other in enumerate(quad_cols):
                copy = remote(
                    landed, landed, quad_send.at[k - 1, child, j], quad_recv.at[k - 1, child, j],
                    row, other,
                )
                copy.start()
                sends.append(copy)

    for j in range(QUAD):
        remote(
            send_pair.at[pl.ds(j * chunk, chunk)], rows_raw.at[1 - core, group, j],
            pair_send.at[j], pair_recv.at[j], pair_row, col,
        ).wait_recv()
    for child in range(2):
        for j in range(QUAD):
            finish_rows(child, group, j)
    remote(own_cols, cols_raw.at[1 - core, group], col_send.at[0], col_recv.at[0], pair_row, col).wait_recv()
    for child in range(2):
        finish_cols(child, group)

    far_sources = [(k, (group + groups - k) % groups) for k in range(1, groups)]

    @pl.when(diag_row // 2 != group)
    def _():
        shared = []
        for k, source in far_sources:
            landed = cols_raw.at[core, source]
            remote(own_cols, landed, col_send.at[k], col_recv.at[k], pair_row, col).wait_recv()
            shared.append(remote(
                landed, landed, fwd_send.at[k - 1], fwd_recv.at[k - 1], pair_row, col
            ))
            shared[-1].start()
        for k, source in far_sources:
            remote(
                own_cols, cols_raw.at[1 - core, source], fwd_send.at[k - 1], fwd_recv.at[k - 1],
                pair_row, col,
            ).wait_recv()
        for copy in shared:
            copy.wait_send()

    @pl.when(row == diag_row)
    def _():
        for source in range(groups):
            for child in range(2):
                @pl.when(2 * source + child != row)
                def _():
                    remote(
                        own_diag, diag_raw.at[child, source], diag_send, diag_recv.at[child, source],
                        pair_row, col,
                    ).wait_recv()
        for source in range(groups):
            for t in range(col_cap):
                total = jnp.zeros((block, block), jnp.float32)
                for child in range(2):
                    _, count = lookup(child, source, t * col_count + col)
                    inside = jnp.maximum(row_iota, col_iota) < count
                    piece = diag_raw[child, source, t * block:(t + 1) * block, :].astype(jnp.float32)
                    total = total + jnp.where(inside, piece, 0.0)
                diag_out[source, t] = total

    @pl.when(row != diag_row)
    def _():
        diag_out[...] = jnp.zeros_like(diag_out)

    for k in range(1, groups):
        source = (group + groups - k) % groups
        for child in range(2):
            for j, other in enumerate(quad_cols):
                landed = rows_raw.at[child, source, other % QUAD]
                remote(
                    landed, landed, quad_send.at[k - 1, child, j], quad_recv.at[k - 1, child, j],
                    row, other,
                ).wait_recv()

    @pl.when(diag_row // 2 == group)
    def _():
        pieces = block // chunk
        shared = []
        for k, source in far_sources:
            for child in range(2):
                for n in range(col_cap * pieces):
                    slot = (n // pieces * col_count + col) // row_count
                    landed = rows_raw.at[child, source, slot * pieces + n % pieces]
                    spot = cols_raw.at[child, source, pl.ds(n * chunk, chunk)]
                    shared.append((landed, spot, remote(
                        landed, spot, own_send.at[k - 1, child, n], own_recv.at[k - 1, child, n],
                        pair_row, col,
                    )))

        @pl.when(row == diag_row)
        def _():
            for landed, spot, copy in shared:
                copy.start()
            for landed, spot, copy in shared:
                spot[...] = landed[...]
            for landed, spot, copy in shared:
                copy.wait_send()

        @pl.when(row != diag_row)
        def _():
            for landed, spot, copy in shared:
                copy.wait_recv()

    for k, source in far_sources:
        for child in range(2):
            finish_cols(child, source)
            for j in range(QUAD):
                finish_rows(child, source, j)

    front_load.wait()
    for copy in sends:
        copy.wait_send()
    for dest, copy in col_away:
        pl.when(diag_row // 2 != dest)(copy.wait_send)

    @pl.when(row != diag_row)
    def _():
        diag_away.wait_send()


def add_kernel(
    row_count, col_count, front_ref, rows_ref, cols_ref, diag_ref, out_ref, staged, out_sem
):
    rows_local = rows_ref.shape[0]
    cols_local, _, block = cols_ref.shape
    halves = block // LANES
    per_row = halves * cols_local
    row = lax.axis_index("row")
    col = lax.axis_index("col")

    def write(a):
        return pltpu.make_async_copy(staged.at[a % 2], out_ref.at[a], out_sem.at[a % 2])

    for a in range(rows_local):
        if a >= 2:
            write(a - 2).wait()
        for b in range(cols_local):
            tile = jnp.dot(rows_ref[a], cols_ref[b], preferred_element_type=jnp.float32)
            for h in range(halves):
                spot = pl.ds(h * cols_local + b, block, stride=per_row)
                staged[a % 2, spot, :] = front_ref[a, spot, :] + tile[:, h * LANES:(h + 1) * LANES]
        row_parent = a * row_count + row

        @pl.when(row_parent % col_count == col)
        def _():
            b = row_parent // col_count
            for h in range(halves):
                spot = pl.ds(h * cols_local + b, block, stride=per_row)
                piece = diag_ref[b, :, h * LANES:(h + 1) * LANES]
                staged[a % 2, spot, :] = staged[a % 2, spot, :] + piece

        write(a).start()
    for a in range(rows_local - 2, rows_local):
        write(a).wait()


def shards(parent_front, generators, diagonal_blocks, coupling, block_map, valid_rows):
    row_count = lax.axis_size("row")
    col_count = lax.axis_size("col")
    groups = row_count // 2
    block, rank = generators.shape[1:]
    rows_local = parent_front.shape[0]
    cols_local = parent_front.shape[2]
    row_cap = rows_local // groups
    col_cap = cols_local // groups
    chunk = row_cap * block // QUAD
    vmem = pl.BlockSpec(memory_space=pltpu.VMEM)
    hbm = pl.BlockSpec(memory_space=pltpu.HBM)
    dma = pltpu.SemaphoreType.DMA
    halves = block // LANES
    per_row = halves * cols_local
    flat = parent_front.reshape(rows_local, block, cols_local, halves, LANES)
    flat = flat.transpose(0, 1, 3, 2, 4).reshape(rows_local, block * per_row, LANES)
    operands = [
        pltpu.with_memory_space_constraint(x, pltpu.HBM)
        for x in (generators, diagonal_blocks, coupling, block_map, valid_rows, flat)
    ]
    rows, cols, diag, front = pl.pallas_call(
        functools.partial(exchange_kernel, row_count, col_count, row_cap, col_cap),
        out_shape=(
            pltpu.VMEM((groups, QUAD, chunk, 2 * rank), jnp.bfloat16),
            pltpu.VMEM((groups, col_cap, 2 * rank, block), jnp.bfloat16),
            pltpu.VMEM((groups, col_cap, block, block), jnp.float32),
            pltpu.VMEM(flat.shape, jnp.float32),
        ),
        in_specs=[hbm] * 6,
        out_specs=(vmem,) * 4,
        scratch_shapes=[
            pltpu.VMEM(generators.shape, jnp.bfloat16),
            pltpu.VMEM(diagonal_blocks.shape, jnp.bfloat16),
            pltpu.VMEM(coupling.shape, jnp.bfloat16),
            pltpu.SMEM(block_map.shape, jnp.int32),
            pltpu.SMEM(valid_rows.shape, jnp.int32),
            dma((5,)),
            dma,
            pltpu.VMEM((groups - 1, 2, chunk, rank), jnp.bfloat16),
            pltpu.VMEM((row_cap * block, rank), jnp.bfloat16),
            pltpu.VMEM((2, groups, QUAD, chunk, rank), jnp.bfloat16),
            pltpu.VMEM((2, groups, col_cap * block, rank), jnp.bfloat16),
            pltpu.VMEM((2, groups, col_cap * block, block), jnp.bfloat16),
            dma((groups - 1, 2)),
            dma((groups - 1, 2)),
            dma((groups - 1, 2, QUAD - 1)),
            dma((groups - 1, 2, QUAD - 1)),
            dma((QUAD,)),
            dma((QUAD,)),
            dma((groups,)),
            dma((groups,)),
            dma((groups - 1,)),
            dma((groups - 1,)),
            dma,
            dma((2, groups)),
            dma((groups - 1, 2, col_cap * block // chunk)),
            dma((groups - 1, 2, col_cap * block // chunk)),
        ],
        compiler_params=pltpu.CompilerParams(
            collective_id=0, has_side_effects=True, vmem_limit_bytes=32 * 1024 * 1024
        ),
    )(*operands)
    rows = rows.reshape(rows_local, block, 2 * rank)
    cols = cols.reshape(cols_local, 2 * rank, block)
    diag = diag.reshape(cols_local, block, block)
    out = pl.pallas_call(
        functools.partial(add_kernel, row_count, col_count),
        out_shape=jax.ShapeDtypeStruct(flat.shape, jnp.float32),
        in_specs=[vmem] * 4,
        out_specs=hbm,
        scratch_shapes=[pltpu.VMEM((2,) + flat.shape[1:], jnp.float32), dma((2,))],
        compiler_params=pltpu.CompilerParams(vmem_limit_bytes=32 * 1024 * 1024),
    )(*(pltpu.with_memory_space_constraint(x, pltpu.VMEM) for x in (front, rows, cols, diag)))
    out = out.reshape(rows_local, block, halves, cols_local, LANES)
    return out.transpose(0, 1, 3, 2, 4).reshape(parent_front.shape)


def solution(mesh):
    in_specs = (
        P(None, "row", None, "col"),
        P("row", None, None),
        P("row", None, None),
        P(),
        P(),
        P(),
    )
    out_specs = P(None, "row", None, "col")
    return jax.shard_map(shards, mesh=mesh, in_specs=in_specs, out_specs=out_specs, check_vma=False)
```
